32 devices in a mesh: seq: 8 (over y, x, core), head: 4 (over z).
Axes of the slice: x: 2, y: 2, z: 4, core: 2. Of those that a mesh axis runs over, the one named last changes fastest.
Arguments:
- queries: bfloat16 [16384, 512], P('seq', 'head'), may hold values from -6 to 6
- keys: bfloat16 [16384, 512], P('seq', 'head'), may hold values from -6 to 6
- values: bfloat16 [16384, 512], P('seq', 'head'), may hold values from -6 to 6
- level_ids: int32 [16384], P('seq'), may hold values from 0 to 63
- level_table: float32 [64, 15], replicated, may hold values from 0 to 4, as said below
- out_cotangent: bfloat16 [16384, 2048], P('seq', 'head'), may hold values from -6 to 6
Outputs:
- attn_out: bfloat16 [16384, 512], P('seq', 'head')
- weight_grad: float32 [2048, 512], P('seq', 'head')
The draws below stay inside these ranges and needn't reach their ends.
Inputs may be any that keep to these rules, and one draw needn't show every extreme that they name: `level_table`: positive coefficients.
All inputs are finite; a program needn't handle non-finite values.
Results may differ from the reference program's by a relative error of at most 0.0043.
Values may be sent and summed in bfloat16 or wider, within the bound.
A program may use at most 64 MiB of HBM per device.

```python
import jax
import jax.numpy as jnp
from jax import lax

D = 2048
HD = 128
NID = 64
TOK_DEV = 2048
HEADS = 4
TOKENS = 16384
LOCAL_BITS = 11
SEQ_BITS = 3
LEVELS = 15
N_SEQ = 8


def draw_level_table(key, part):
    spread = jax.random.uniform(key, (NID, LEVELS), jnp.float32, -0.7, 0.7)
    level_depth = jnp.maximum(jnp.arange(LEVELS) - 1, 0).astype(jnp.float32)
    return jnp.exp(spread) * jnp.exp2(-0.5 * level_depth)[None, :]


def plant(entries, stream_key, low, largest):
    place = [jax.random.randint(jax.random.fold_in(stream_key, axis), (), 0, length) for axis, length in enumerate(entries.shape)]
    longest = entries.shape.index(max(entries.shape))
    next_to = place[:longest] + [(place[longest] + 1) % entries.shape[longest]] + place[longest + 1:]
    return entries.at[tuple(place)].set(low).at[tuple(next_to)].set(largest)


def with_spikes(values, key, source, target, blocks, factor):
    def block_of(dim):
        return (jnp.arange(values.shape[dim]) // (values.shape[dim] // blocks)).reshape((-1,) + (1,) * (values.ndim - 1 - dim))

    near = jax.random.permutation(key, blocks)[block_of(target)]
    second = (block_of(target) + blocks // 2) % blocks
    return jnp.where((block_of(source) == near) | (block_of(source) == second), factor * values, values)


def level_of(stream_key, dims, pieces, low, high):
    def one(dim, blocks):
        draws = jax.random.uniform(jax.random.fold_in(jax.random.fold_in(stream_key, 6), dim), (blocks,), jnp.float32, low / len(pieces), high / len(pieces))
        return jnp.repeat(jnp.exp(draws), dims[dim] // blocks).reshape((-1,) + (1,) * (len(dims) - dim - 1))

    factor_of = one(*pieces[0])
    for cut in pieces[1:]:
        factor_of = factor_of * one(*cut)
    return factor_of


def scatter_about(stream_key, dims, deviation, bound, cuts=(), kind=jnp.bfloat16):
    values = deviation * jax.random.normal(stream_key, dims, jnp.float32)
    if cuts:
        values = values * level_of(stream_key, dims, cuts, -0.22, 0.18)
    return jnp.clip(values, -bound, bound).astype(kind)


def bell_draw_with(rng, shape, width, most, split, heavy, held_as=jnp.bfloat16):
    result = width * jax.random.normal(rng, shape, jnp.float32)
    if split:
        result = result * level_of(rng, shape, split, -0.22, 0.18)
    return jnp.clip(with_spikes(result, jax.random.fold_in(rng, 3), *heavy), -most, most).astype(held_as)


def setup_inputs(seed: int = 0) -> dict:
    arg_keys = jax.random.split(jax.random.key(seed), 7)
    queries = scatter_about(arg_keys[0], (TOKENS, HEADS * HD), 1.0, 6.0, ((0, 8), (1, 4)))
    keys = scatter_about(arg_keys[1], (TOKENS, HEADS * HD), 1.0, 6.0, ((0, 8), (1, 4)))
    values = scatter_about(arg_keys[2], (TOKENS, HEADS * HD), 1.0, 6.0, ((0, 8), (1, 4)))
    level_ids = plant(jax.random.randint(arg_keys[3], (TOKENS,), 0, NID), jax.random.fold_in(arg_keys[3], 1), 0, NID - 1).astype(jnp.int32)
    level_table = draw_level_table(jax.random.fold_in(arg_keys[6], 71), 0)
    out_cotangent = bell_draw_with(arg_keys[5], (TOKENS, D), 1.0, 6.0, ((0, 8), (1, 4)), (0, 1, 8, 2.0))
    return dict(queries=queries, keys=keys, values=values, level_ids=level_ids, level_table=level_table, out_cotangent=out_cotangent)


EPSILON = 1e-06
HIGHEST = lax.Precision.HIGHEST

def level_index(row_pos, col_pos, bit_count):
    xor_value = jnp.bitwise_xor(row_pos, col_pos)
    levels = jnp.zeros(xor_value.shape, jnp.int32)
    for shift_by in range(bit_count):
        levels = levels + (jnp.right_shift(xor_value, shift_by) > 0).astype(jnp.int32)
    return levels

def split_heads(array):
    return array.reshape(N_SEQ, TOK_DEV, HEADS, HD).transpose(2, 0, 1, 3)

def reference(queries, keys, values, level_ids, level_table, out_cotangent):
    coeff = level_table[level_ids].reshape(N_SEQ, TOK_DEV, LEVELS)
    position = jnp.arange(TOK_DEV, dtype=jnp.int32)
    levels = level_index(position[:, None], position[None, :], LOCAL_BITS)
    causal = position[None, :] <= position[:, None]

    def block_weights(block_coeff):
        weights = jnp.zeros((TOK_DEV, TOK_DEV), jnp.float32)
        for level in range(LOCAL_BITS + 1):
            weights = weights + jnp.where(levels == level, block_coeff[:, level:level + 1], 0.0)
        return jnp.where(causal, weights, 0.0)
    all_weights = lax.map(block_weights, coeff)
    owner = jnp.arange(N_SEQ, dtype=jnp.int32)
    apart = jnp.bitwise_xor(owner[:, None], owner[None, :])
    earlier = owner[None, :] < owner[:, None]
    sibling = jnp.stack([((jnp.right_shift(apart, level) == 1) & earlier).astype(jnp.float32) for level in range(SEQ_BITS)])
    cross_coeff = coeff[:, :, LOCAL_BITS + 1:]

    def one_head(parts):
        query_blocks, key_blocks, value_blocks = parts

        def one_block(items):
            query, key_block, value, weights = items
            scores = jnp.dot(query, key_block.T, preferred_element_type=jnp.float32)
            mixed = (weights * scores).astype(jnp.bfloat16)
            local = jnp.dot(mixed, value, preferred_element_type=jnp.float32)
            state = jnp.dot(key_block.T, value, preferred_element_type=jnp.float32)
            return (local, state)
        local, states = lax.map(one_block, (query_blocks, key_blocks, value_blocks, all_weights))
        level_states = jnp.einsum('jcb,bde->jcde', sibling, states, precision=HIGHEST)
        readout = jnp.einsum('cti,jcie->ctje', query_blocks.astype(jnp.float32), level_states, precision=HIGHEST)
        cross = lax.optimization_barrier(jnp.sum(readout * cross_coeff[:, :, :, None], axis=2))
        total = local + cross
        normed = total * lax.rsqrt(lax.optimization_barrier(jnp.mean(total * total, axis=-1, keepdims=True)) + EPSILON)
        return normed.astype(jnp.bfloat16)
    heads_out = lax.map(one_head, (split_heads(queries), split_heads(keys), split_heads(values)))
    attn_out = heads_out.transpose(1, 2, 0, 3).reshape(TOKENS, HEADS * HD)
    weight_grad = jnp.dot(out_cotangent.T, attn_out, preferred_element_type=jnp.float32) * TOKENS ** (-0.5)
    return (attn_out, weight_grad)
```

```python
import functools

import jax
import jax.numpy as jnp
from jax import lax
from jax.experimental import pallas as pl
from jax.experimental.pallas import tpu as pltpu
from jax.sharding import PartitionSpec as P

EPSILON = 1e-06
TILE = 128
CHUNKS = 4
MESH = pl.DeviceIdType.MESH
F32 = jnp.float32
BF16 = jnp.bfloat16


def dot(a, b, ca, cb):
    return lax.dot_general(a, b, (((ca,), (cb,)), ((), ())), preferred_element_type=F32)


def tile_levels(tile):
    row = lax.broadcasted_iota(jnp.int32, (tile, tile), 0)
    col = lax.broadcasted_iota(jnp.int32, (tile, tile), 1)
    apart = jnp.bitwise_xor(row, col)
    levels = jnp.zeros((tile, tile), jnp.int32)
    for bit in range(tile.bit_length() - 1):
        levels = levels + (jnp.right_shift(apart, bit) > 0).astype(jnp.int32)
    return jnp.where(col <= row, levels, -1)


def kernel(
    n_seq, n_head,
    q_hbm, k_hbm, v_hbm, ids_ref, table_ref, cot_hbm,
    attn_hbm, grad_ref,
    q_ref, k_ref, v_ref, cot_ref, levels_ref, coeff_ref, total_ref, sib_ref,
    state_ref, states_ref, flat_ref, attn_ref, gather_ref, acc_ref,
    share_ref, shares_ref, final_ref, finals_ref,
    load_sem, out_sem, state_send, state_recv, ring_send, ring_recv,
    share_send, share_recv, final_send, final_recv,
):
    seq, head = lax.axis_index("seq"), lax.axis_index("head")
    block_len, head_dim = q_ref.shape
    width = cot_ref.shape[1]
    tiles = block_len // TILE
    chunk = block_len // CHUNKS
    tile_bits = TILE.bit_length() - 1
    local_bits = block_len.bit_length() - 1
    inner = local_bits - tile_bits
    seq_bits = n_seq.bit_length() - 1
    owners = n_seq // n_head
    rows_per = max(16, head_dim // n_seq)
    reducers = head_dim // rows_per
    piece = finals_ref.shape[1]
    scale = (block_len * n_seq) ** (-0.5)

    loads = [
        pltpu.make_async_copy(src, dst, load_sem.at[i])
        for i, (src, dst) in enumerate(
            [(k_hbm, k_ref), (v_hbm, v_ref), (q_hbm, q_ref), (cot_hbm, cot_ref)]
        )
    ]
    for load in loads:
        load.start()

    barrier = pltpu.get_barrier_semaphore()
    me = seq * n_head + head

    def greet(step, carry):
        other = lax.rem(me + step, n_seq * n_head)
        pl.semaphore_signal(
            barrier, inc=1, device_id=(other // n_head, lax.rem(other, n_head)),
            device_id_type=MESH,
        )
        return carry

    lax.fori_loop(1, n_seq * n_head, greet, 0)

    table = table_ref[...]
    high = table.astype(BF16)
    rest = table - high.astype(F32)
    mid = rest.astype(BF16)
    low = (rest - mid.astype(F32)).astype(BF16)
    table3 = jnp.concatenate([high, mid, low], axis=0)
    levels_ref[...] = tile_levels(TILE)

    loads[0].wait()
    loads[1].wait()
    nodes = [
        dot(k_ref[pl.ds(i * TILE, TILE), :], v_ref[pl.ds(i * TILE, TILE), :], 0, 0)
        for i in range(tiles)
    ]
    for bit in range(inner):
        for i in range(tiles):
            place = (i >> bit) ^ 1
            value = nodes[place].astype(BF16) if (i >> bit) & 1 else jnp.zeros((head_dim, head_dim), BF16)
            sib_ref[i, :, pl.ds(bit * head_dim, head_dim)] = value
        nodes = [nodes[2 * i] + nodes[2 * i + 1] for i in range(len(nodes) // 2)]
    state_ref[...] = nodes[0].astype(BF16)

    pl.semaphore_wait(barrier, n_seq * n_head - 1)

    def state_copy(target):
        return pltpu.make_async_remote_copy(
            src_ref=state_ref, dst_ref=states_ref.at[seq],
            send_sem=state_send.at[target], recv_sem=state_recv.at[seq],
            device_id=(target, head), device_id_type=MESH,
        )

    for target in range(1, n_seq):
        @pl.when(seq < target)
        def _():
            state_copy(target).start()

    loads[2].wait()

    def local_tile(i, carry):
        rows = pl.ds(pl.multiple_of(i * TILE, TILE), TILE)
        row_ids = lax.broadcasted_iota(jnp.int32, (table.shape[0], TILE), 0)
        onehot = (row_ids == ids_ref[:, rows]).astype(F32).astype(BF16)
        coeff = dot(jnp.concatenate([onehot] * 3, axis=0), table3, 0, 0)
        coeff_ref[rows, :] = coeff
        levels = levels_ref[...]
        weights = jnp.zeros((TILE, TILE), F32)
        for level in range(tile_bits + 1):
            weights = jnp.where(levels == level, coeff[:, level : level + 1], weights)
        query = q_ref[rows, :]
        scores = dot(query, k_ref[rows, :], 1, 1)
        total = dot((weights * scores).astype(BF16), v_ref[rows, :], 1, 0)
        readout = dot(query, sib_ref[i], 1, 0)
        for bit in range(inner):
            level = tile_bits + 1 + bit
            total += coeff[:, level : level + 1] * readout[:, bit * head_dim : (bit + 1) * head_dim]
        total_ref[rows, :] = total
        return carry

    lax.fori_loop(0, tiles, local_tile, 0, unroll=4)

    for bit in range(seq_bits):
        span = 2**bit
        node = seq // span
        columns = pl.ds(bit * head_dim, head_dim)

        @pl.when(lax.rem(node, 2) == 1)
        def _():
            total = jnp.zeros((head_dim, head_dim), F32)
            for offset in range(span):
                source = (node - 1) * span + offset
                pltpu.make_async_remote_copy(
                    src_ref=state_ref, dst_ref=states_ref.at[source],
                    send_sem=state_send.at[0], recv_sem=state_recv.at[source],
                    device_id=(source, head), device_id_type=MESH,
                ).wait_recv()
                total += states_ref[source].astype(F32)
            upper = total.astype(BF16)
            flat_ref[pl.ds(0, head_dim), columns] = upper
            flat_ref[pl.ds(head_dim, head_dim), columns] = (total - upper.astype(F32)).astype(BF16)

        @pl.when(lax.rem(node, 2) == 0)
        def _():
            flat_ref[:, columns] = jnp.zeros((2 * head_dim, head_dim), BF16)

    right, left = lax.rem(head + 1, n_head), lax.rem(head + n_head - 1, n_head)

    def reach(way, c):
        return n_head // 2 if (c < CHUNKS // 2) == (way == 0) else (n_head - 1) // 2

    def ring_copy(way, distance, c):
        origin = lax.rem(head + (n_head - distance if way == 0 else distance), n_head)
        return pltpu.make_async_remote_copy(
            src_ref=gather_ref.at[origin, c], dst_ref=gather_ref.at[origin, c],
            send_sem=ring_send.at[way, distance, c], recv_sem=ring_recv.at[way, distance, c],
            device_id=(seq, right if way == 0 else left), device_id_type=MESH,
        )

    def ring_arrival(way, distance, c):
        origin = lax.rem(head + (n_head - distance if way == 0 else distance), n_head)
        pltpu.make_async_remote_copy(
            src_ref=gather_ref.at[origin, c], dst_ref=gather_ref.at[origin, c],
            send_sem=ring_send.at[way, distance - 1, c], recv_sem=ring_recv.at[way, distance - 1, c],
            device_id=(seq, right if way == 0 else left), device_id_type=MESH,
        ).wait_recv()
        return origin

    def attn_tile(first):
        def one(i, carry):
            rows = pl.ds(pl.multiple_of(first * chunk + i * TILE, TILE), TILE)
            query = q_ref[rows, :]
            readout = dot(jnp.concatenate([query, query], axis=1), flat_ref[...], 1, 0)
            coeff = coeff_ref[rows, :]
            cross = jnp.zeros((TILE, head_dim), F32)
            for bit in range(seq_bits):
                level = local_bits + 1 + bit
                cross += coeff[:, level : level + 1] * readout[:, bit * head_dim : (bit + 1) * head_dim]
            total = total_ref[rows, :] + cross
            normed = total * lax.rsqrt(jnp.mean(total * total, axis=1, keepdims=True) + EPSILON)
            attn_ref[rows, :] = normed.astype(BF16)
            gather_ref[head, first, :, pl.ds(pl.multiple_of(i * TILE, TILE), TILE)] = normed.T.astype(BF16)
            return carry
        return one

    for c in range(CHUNKS):
        lax.fori_loop(0, chunk // TILE, attn_tile(c), 0, unroll=True)
        for way in range(2):
            if reach(way, c) > 0:
                ring_copy(way, 0, c).start()

    attn_copy = pltpu.make_async_copy(attn_ref, attn_hbm, out_sem.at[0])
    attn_copy.start()

    def multiply(origin, c, fresh):
        part = dot(gather_ref[origin, c], cot_ref[pl.ds(c * chunk, chunk), :], 1, 0)
        if fresh:
            acc_ref[origin] = part
        else:
            acc_ref[origin] += part

    def share_copy(origin, target):
        return pltpu.make_async_remote_copy(
            src_ref=share_ref.at[origin, pl.ds(target * rows_per, rows_per), :],
            dst_ref=shares_ref.at[origin, seq],
            send_sem=share_send.at[origin, target], recv_sem=share_recv.at[origin, seq],
            device_id=(target, head), device_id_type=MESH,
        )

    def send_share(origin):
        share_ref[origin] = (acc_ref[origin] * scale).astype(BF16)
        for target in range(reducers):
            @pl.when(seq != target)
            def _():
                share_copy(origin, target).start()

    def final_copy(origin, owner):
        columns = pl.ds(owner * piece if piece < width else 0, piece)
        return pltpu.make_async_remote_copy(
            src_ref=final_ref.at[origin, :, columns] if piece < width else final_ref.at[origin],
            dst_ref=finals_ref.at[pl.ds(pl.multiple_of(seq * rows_per, rows_per), rows_per), :],
            send_sem=final_send.at[origin, owner], recv_sem=final_recv.at[seq],
            device_id=(head * owners + owner, origin), device_id_type=MESH,
        )

    def is_self(origin, owner):
        return jnp.logical_and(head * owners + owner == seq, origin == head)

    def reduce_share(origin):
        @pl.when(seq < reducers)
        def _():
            mine = pl.ds(pl.multiple_of(seq * rows_per, rows_per), rows_per)
            final_ref[origin] = acc_ref[origin, mine, :] * scale

            def add(step, carry):
                source = lax.rem(seq + step, n_seq)
                pltpu.make_async_remote_copy(
                    src_ref=share_ref.at[origin, pl.ds(0, rows_per), :],
                    dst_ref=shares_ref.at[origin, source],
                    send_sem=share_send.at[origin, 0], recv_sem=share_recv.at[origin, source],
                    device_id=(source, head), device_id_type=MESH,
                ).wait_recv()
                final_ref[origin] += shares_ref[origin, source].astype(F32)
                return carry

            lax.fori_loop(1, n_seq, add, 0)
            for owner in range(owners):
                @pl.when(jnp.logical_not(is_self(origin, owner)))
                def _():
                    final_copy(origin, owner).start()

                @pl.when(is_self(origin, owner))
                def _():
                    whole = final_ref[origin]
                    start = owner * piece if piece < width else 0
                    finals_ref[mine, :] = whole[:, start : start + piece]

    loads[3].wait()
    for c in range(CHUNKS):
        multiply(head, c, c == 0)
    send_share(head)
    waiting = [head]
    for distance in range(1, n_head // 2 + 1):
        met = []
        for c in range(CHUNKS):
            for way in range(2):
                if distance <= reach(way, c):
                    origin = ring_arrival(way, distance, c)
                    if distance < reach(way, c):
                        ring_copy(way, distance, c).start()
                    side = way if 2 * distance < n_head else 0
                    multiply(origin, c, side not in met)
                    met.append(side)
        done = [lax.rem(head + n_head - distance, n_head)]
        if 2 * distance < n_head:
            done.append(lax.rem(head + distance, n_head))
        for origin in done:
            send_share(origin)
        for origin in waiting:
            reduce_share(origin)
        waiting = done
    for origin in waiting:
        reduce_share(origin)

    home = seq // owners
    for source in range(reducers):
        @pl.when(jnp.logical_not(jnp.logical_and(seq == source, head == home)))
        def _():
            pltpu.make_async_remote_copy(
                src_ref=final_ref.at[0, :, pl.ds(0, piece)] if piece < width else final_ref.at[0],
                dst_ref=finals_ref.at[pl.ds(source * rows_per, rows_per), :],
                send_sem=final_send.at[0, 0], recv_sem=final_recv.at[source],
                device_id=(source, home), device_id_type=MESH,
            ).wait_recv()
    if grad_ref.shape[1] == piece:
        grad_ref[...] = finals_ref[...]
    else:
        per = grad_ref.shape[1]
        for owner in range(owners):
            @pl.when(lax.rem(seq, owners) == owner)
            def _():
                grad_ref[...] = finals_ref[...][:, owner * per : (owner + 1) * per]

    for target in range(1, n_seq):
        @pl.when(seq < target)
        def _():
            state_copy(target).wait_send()
    for c in range(CHUNKS):
        for way in range(2):
            for distance in range(reach(way, c)):
                ring_copy(way, distance, c).wait_send()
    for origin in range(n_head):
        for target in range(reducers):
            @pl.when(seq != target)
            def _():
                share_copy(origin, target).wait_send()

        @pl.when(seq < reducers)
        def _():
            for owner in range(owners):
                @pl.when(jnp.logical_not(is_self(origin, owner)))
                def _():
                    final_copy(origin, owner).wait_send()
    attn_copy.wait()


def body(n_seq, n_head, queries, keys, values, level_ids, level_table, out_cotangent):
    block_len, head_dim = queries.shape
    width = out_cotangent.shape[1]
    per = width * n_head // n_seq
    piece = per if per % 128 == 0 else width
    seq_bits = n_seq.bit_length() - 1
    inner = (block_len // TILE).bit_length() - 1
    rows_per = max(16, head_dim // n_seq)
    reducers = head_dim // rows_per
    steps = max(1, n_head // 2)
    dma = pltpu.SemaphoreType.DMA
    vmem = pl.BlockSpec(memory_space=pltpu.VMEM)
    hbm = pl.BlockSpec(memory_space=pl.ANY)
    attn_out, grad = pl.pallas_call(
        functools.partial(kernel, n_seq, n_head),
        out_shape=(
            jax.ShapeDtypeStruct((block_len, head_dim), BF16),
            jax.ShapeDtypeStruct((head_dim, per), F32),
        ),
        in_specs=[hbm, hbm, hbm, vmem, vmem, hbm],
        out_specs=(hbm, vmem),
        scratch_shapes=[
            pltpu.VMEM((block_len, head_dim), BF16),
            pltpu.VMEM((block_len, head_dim), BF16),
            pltpu.VMEM((block_len, head_dim), BF16),
            pltpu.VMEM((block_len, width), BF16),
            pltpu.VMEM((TILE, TILE), jnp.int32),
            pltpu.VMEM((block_len, level_table.shape[1]), F32),
            pltpu.VMEM((block_len, head_dim), F32),
            pltpu.VMEM((block_len // TILE, head_dim, inner * head_dim), BF16),
            pltpu.VMEM((head_dim, head_dim), BF16),
            pltpu.VMEM((n_seq, head_dim, head_dim), BF16),
            pltpu.VMEM((2 * head_dim, seq_bits * head_dim), BF16),
            pltpu.VMEM((block_len, head_dim), BF16),
            pltpu.VMEM((n_head, CHUNKS, head_dim, block_len // CHUNKS), BF16),
            pltpu.VMEM((n_head, head_dim, width), F32),
            pltpu.VMEM((n_head, head_dim, width), BF16),
            pltpu.VMEM((n_head, n_seq, rows_per, width), BF16),
            pltpu.VMEM((n_head, rows_per, width), F32),
            pltpu.VMEM((head_dim, piece), F32),
            dma((4,)),
            dma((1,)),
            dma((n_seq,)),
            dma((n_seq,)),
            dma((2, steps, CHUNKS)),
            dma((2, steps, CHUNKS)),
            dma((n_head, reducers)),
            dma((n_head, n_seq)),
            dma((n_head, n_seq // n_head)),
            dma((reducers,)),
        ],
        compiler_params=pltpu.CompilerParams(
            collective_id=0, has_side_effects=True, vmem_limit_bytes=60 * 2**20
        ),
    )(queries, keys, values, level_ids[None, :], level_table, out_cotangent)
    return attn_out, grad.T


def solution(mesh):
    in_specs = (
        P("seq", "head"),
        P("seq", "head"),
        P("seq", "head"),
        P("seq"),
        P(),
        P("seq", "head"),
    )
    out_specs = (P("seq", "head"), P("seq", "head"))
    return jax.shard_map(
        functools.partial(body, mesh.shape["seq"], mesh.shape["head"]),
        mesh=mesh, in_specs=in_specs, out_specs=out_specs, check_vma=False,
    )
```

```python
import functools

import jax
import jax.numpy as jnp
from jax import lax
from jax.experimental import pallas as pl
from jax.experimental.pallas import tpu as pltpu
from jax.sharding import PartitionSpec as P

EPSILON = 1e-06
TILE = 128
CHUNKS = 8
KEEP = 5
MESH = pl.DeviceIdType.MESH
F32 = jnp.float32
BF16 = jnp.bfloat16


def dot(a, b, ca, cb):
    return lax.dot_general(a, b, (((ca,), (cb,)), ((), ())), preferred_element_type=F32)


def tile_levels(tile):
    row = lax.broadcasted_iota(jnp.int32, (tile, tile), 0)
    col = lax.broadcasted_iota(jnp.int32, (tile, tile), 1)
    apart = jnp.bitwise_xor(row, col)
    levels = jnp.zeros((tile, tile), jnp.int32)
    for bit in range(tile.bit_length() - 1):
        levels = levels + (jnp.right_shift(apart, bit) > 0).astype(jnp.int32)
    return jnp.where(col <= row, levels, -1)


def kernel(
    n_seq, n_head,
    q_hbm, k_hbm, v_hbm, ids_ref, table_ref, cot_hbm,
    attn_hbm, grad_ref,
    q_ref, k_ref, v_ref, cot_ref, levels_ref, coeff_ref, total_ref, sib_ref,
    state_ref, states_ref, flat_ref, attn_ref, gather_ref, acc_ref,
    share_ref, shares_ref, final_ref, finals_ref, help_ref,
    load_sem, out_sem, state_send, state_recv, ring_send, ring_recv,
    share_send, share_recv, final_send, final_recv, help_send, help_recv,
):
    seq, head = lax.axis_index("seq"), lax.axis_index("head")
    block_len, head_dim = q_ref.shape
    width = cot_ref.shape[1]
    tiles = block_len // TILE
    chunk = block_len // CHUNKS
    tile_bits = TILE.bit_length() - 1
    local_bits = block_len.bit_length() - 1
    inner = local_bits - tile_bits
    seq_bits = n_seq.bit_length() - 1
    owners = n_seq // n_head
    rows_per = max(16, head_dim // n_seq)
    reducers = head_dim // rows_per
    piece = finals_ref.shape[2]
    last = n_head - 1
    keep = CHUNKS - help_ref.shape[0] if n_head >= 4 else CHUNKS
    scale = (block_len * n_seq) ** (-0.5)

    loads = [
        pltpu.make_async_copy(src, dst, load_sem.at[i])
        for i, (src, dst) in enumerate(
            [(k_hbm, k_ref), (v_hbm, v_ref), (q_hbm, q_ref), (cot_hbm, cot_ref)]
        )
    ]
    for load in loads:
        load.start()

    barrier = pltpu.get_barrier_semaphore()
    me = seq * n_head + head

    def greet(step, carry):
        other = lax.rem(me + step, n_seq * n_head)
        pl.semaphore_signal(
            barrier, inc=1, device_id=(other // n_head, lax.rem(other, n_head)),
            device_id_type=MESH,
        )
        return carry

    lax.fori_loop(1, n_seq * n_head, greet, 0)

    table = table_ref[...]
    high = table.astype(BF16)
    rest = table - high.astype(F32)
    mid = rest.astype(BF16)
    low = (rest - mid.astype(F32)).astype(BF16)
    table3 = jnp.concatenate([high, mid, low], axis=1)
    levels_ref[...] = tile_levels(TILE)

    loads[0].wait()
    loads[1].wait()
    nodes = [
        dot(k_ref[pl.ds(i * TILE, TILE), :], v_ref[pl.ds(i * TILE, TILE), :], 0, 0)
        for i in range(tiles)
    ]
    for bit in range(inner):
        for i in range(tiles):
            place = (i >> bit) ^ 1
            value = nodes[place].astype(BF16) if (i >> bit) & 1 else jnp.zeros((head_dim, head_dim), BF16)
            sib_ref[i, :, pl.ds(bit * head_dim, head_dim)] = value
        nodes = [nodes[2 * i] + nodes[2 * i + 1] for i in range(len(nodes) // 2)]
    state_ref[...] = nodes[0].astype(BF16)

    pl.semaphore_wait(barrier, n_seq * n_head - 1)

    def state_copy(target):
        return pltpu.make_async_remote_copy(
            src_ref=state_ref, dst_ref=states_ref.at[seq],
            send_sem=state_send.at[target], recv_sem=state_recv.at[seq],
            device_id=(target, head), device_id_type=MESH,
        )

    for target in range(1, n_seq):
        @pl.when(seq < target)
        def _():
            state_copy(target).start()

    right, left = lax.rem(head + 1, n_head), lax.rem(head + n_head - 1, n_head)
    places = (head, last - head)

    def limit(c):
        return jnp.where(c < keep, last, last - 1)

    def help_copy(way, c):
        return pltpu.make_async_remote_copy(
            src_ref=cot_hbm.at[pl.ds(c * chunk, chunk), :], dst_ref=help_ref.at[c - keep],
            send_sem=help_send.at[c - keep], recv_sem=help_recv.at[c - keep],
            device_id=(seq, left if way == 0 else right), device_id_type=MESH,
        )

    for way in range(2):
        @pl.when(places[way] == last)
        def _():
            for c in range(keep, CHUNKS):
                help_copy(way, c).start()

    acc_ref[...] = jnp.zeros_like(acc_ref)

    loads[2].wait()

    def local_tile(i, carry):
        rows = pl.ds(pl.multiple_of(i * TILE, TILE), TILE)
        row_ids = lax.broadcasted_iota(jnp.int32, (table.shape[1], TILE), 0)
        onehot = (row_ids == ids_ref[:, rows]).astype(F32).astype(BF16)
        coeff = dot(jnp.concatenate([onehot] * 3, axis=0), table3, 0, 1)
        coeff_ref[rows, :] = coeff
        levels = levels_ref[...]
        weights = jnp.zeros((TILE, TILE), F32)
        for level in range(tile_bits + 1):
            weights = jnp.where(levels == level, coeff[:, level : level + 1], weights)
        query = q_ref[rows, :]
        scores = dot(query, k_ref[rows, :], 1, 1)
        total = dot((weights * scores).astype(BF16), v_ref[rows, :], 1, 0)
        readout = dot(query, sib_ref[i], 1, 0)
        for bit in range(inner):
            level = tile_bits + 1 + bit
            total += coeff[:, level : level + 1] * readout[:, bit * head_dim : (bit + 1) * head_dim]
        total_ref[rows, :] = total
        return carry

    lax.fori_loop(0, tiles, local_tile, 0, unroll=4)

    for bit in range(seq_bits):
        span = 2**bit
        node = seq // span
        columns = pl.ds(bit * head_dim, head_dim)

        @pl.when(lax.rem(node, 2) == 1)
        def _():
            total = jnp.zeros((head_dim, head_dim), F32)
            for offset in range(span):
                source = (node - 1) * span + offset
                pltpu.make_async_remote_copy(
                    src_ref=state_ref, dst_ref=states_ref.at[source],
                    send_sem=state_send.at[0], recv_sem=state_recv.at[source],
                    device_id=(source, head), device_id_type=MESH,
                ).wait_recv()
                total += states_ref[source].astype(F32)
            upper = total.astype(BF16)
            flat_ref[pl.ds(0, head_dim), columns] = upper
            flat_ref[pl.ds(head_dim, head_dim), columns] = (total - upper.astype(F32)).astype(BF16)

        @pl.when(lax.rem(node, 2) == 0)
        def _():
            flat_ref[:, columns] = jnp.zeros((2 * head_dim, head_dim), BF16)

    def origin_of(way, distance):
        return lax.rem(head + (n_head - distance if way == 0 else distance), n_head)

    def ring_copy(way, distance, c):
        origin = origin_of(way, distance)
        return pltpu.make_async_remote_copy(
            src_ref=gather_ref.at[origin, c], dst_ref=gather_ref.at[origin, c],
            send_sem=ring_send.at[way, distance, c], recv_sem=ring_recv.at[way, distance, c],
            device_id=(seq, right if way == 0 else left), device_id_type=MESH,
        )

    def ring_arrival(way, distance, c):
        origin = origin_of(way, distance)
        return pltpu.make_async_remote_copy(
            src_ref=gather_ref.at[origin, c], dst_ref=gather_ref.at[origin, c],
            send_sem=ring_send.at[way, distance - 1, c], recv_sem=ring_recv.at[way, distance - 1, c],
            device_id=(seq, right if way == 0 else left), device_id_type=MESH,
        )

    def attn_tile(first):
        def one(i, carry):
            rows = pl.ds(pl.multiple_of(first * chunk + i * TILE, TILE), TILE)
            query = q_ref[rows, :]
            readout = dot(jnp.concatenate([query, query], axis=1), flat_ref[...], 1, 0)
            coeff = coeff_ref[rows, :]
            cross = jnp.zeros((TILE, head_dim), F32)
            for bit in range(seq_bits):
                level = local_bits + 1 + bit
                cross += coeff[:, level : level + 1] * readout[:, bit * head_dim : (bit + 1) * head_dim]
            total = total_ref[rows, :] + cross
            normed = total * lax.rsqrt(jnp.mean(total * total, axis=1, keepdims=True) + EPSILON)
            attn_ref[rows, :] = normed.astype(BF16)
            gather_ref[head, first, :, pl.ds(pl.multiple_of(i * TILE, TILE), TILE)] = normed.T.astype(BF16)
            return carry
        return one

    for c in range(CHUNKS):
        lax.fori_loop(0, chunk // TILE, attn_tile(c), 0, unroll=True)
        for way in range(2):
            @pl.when(places[way] + 1 <= limit(c))
            def _():
                ring_copy(way, 0, c).start()

    attn_copy = pltpu.make_async_copy(attn_ref, attn_hbm, out_sem.at[0])
    attn_copy.start()

    def multiply(origin, c):
        rows = pl.ds(pl.multiple_of(c * chunk, chunk), chunk)
        acc_ref[origin] += dot(gather_ref[origin, c], cot_ref[rows, :], 1, 0)

    def multiply_help(origin, c):
        acc_ref[n_head + origin] += dot(gather_ref[origin, c], help_ref[c - keep], 1, 0)

    def share_copy(origin, target):
        return pltpu.make_async_remote_copy(
            src_ref=share_ref.at[origin, pl.ds(target * rows_per, rows_per), :],
            dst_ref=shares_ref.at[origin, seq],
            send_sem=share_send.at[origin, target], recv_sem=share_recv.at[origin, seq],
            device_id=(target, head), device_id_type=MESH,
        )

    def send_share(origin):
        share_ref[origin] = (acc_ref[origin] * scale).astype(BF16)
        for target in range(reducers):
            @pl.when(seq != target)
            def _():
                share_copy(origin, target).start()

    def final_copy(slot, block, origin, kind, owner):
        columns = pl.ds(owner * piece if piece < width else 0, piece)
        return pltpu.make_async_remote_copy(
            src_ref=final_ref.at[slot, :, columns] if piece < width else final_ref.at[slot],
            dst_ref=finals_ref.at[kind, pl.ds(pl.multiple_of(seq * rows_per, rows_per), rows_per), :],
            send_sem=final_send.at[slot, owner], recv_sem=final_recv.at[kind, seq],
            device_id=(block * owners + owner, origin), device_id_type=MESH,
        )

    def is_self(block, origin, owner):
        return jnp.logical_and(block * owners + owner == seq, origin == head)

    def reduce_share(slot, block, origin, kind):
        @pl.when(seq < reducers)
        def _():
            mine = pl.ds(pl.multiple_of(seq * rows_per, rows_per), rows_per)
            final_ref[slot] = acc_ref[slot, mine, :] * scale

            def add(step, carry):
                source = lax.rem(seq + step, n_seq)
                pltpu.make_async_remote_copy(
                    src_ref=share_ref.at[slot, pl.ds(0, rows_per), :],
                    dst_ref=shares_ref.at[slot, source],
                    send_sem=share_send.at[slot, 0], recv_sem=share_recv.at[slot, source],
                    device_id=(source, head), device_id_type=MESH,
                ).wait_recv()
                final_ref[slot] += shares_ref[slot, source].astype(F32)
                return carry

            lax.fori_loop(1, n_seq, add, 0)
            for owner in range(owners):
                @pl.when(jnp.logical_not(is_self(block, origin, owner)))
                def _():
                    final_copy(slot, block, origin, kind, owner).start()

                @pl.when(is_self(block, origin, owner))
                def _():
                    whole = final_ref[slot]
                    start = owner * piece if piece < width else 0
                    finals_ref[kind, mine, :] = whole[:, start : start + piece]

    loads[3].wait()

    def own_chunk(c, carry):
        multiply(head, c)
        return carry

    lax.fori_loop(0, CHUNKS, own_chunk, 0)
    send_share(head)
    every = [(head >= 0, head, head, head, 0)]
    waiting = list(every)
    helps = n_head >= 4
    for distance in range(1, n_head):
        def arrivals(c, carry):
            for way in range(2):
                place = places[way]

                @pl.when(jnp.logical_and(place >= distance, place <= limit(c)))
                def _():
                    ring_arrival(way, distance, c).wait_recv()
                    if distance < last:
                        @pl.when(place + 1 <= limit(c))
                        def _():
                            ring_copy(way, distance, c).start()
                    origin = origin_of(way, distance)
                    multiply(origin, c)
                    if helps and distance < last:
                        @pl.when(jnp.logical_and(place == last - 1, c >= keep))
                        def _():
                            if distance == 1:
                                help_copy(way, c).wait_recv()
                                multiply_help(head, c)
                            multiply_help(origin, c)
            return carry

        lax.fori_loop(0, CHUNKS, arrivals, 0)
        done = []
        for way in range(2):
            origin, place = origin_of(way, distance), places[way]
            done.append((place >= distance, origin, head, origin, 0))
            if helps and distance < last:
                block = last if way == 0 else 0
                helper = place == last - 1
                if distance == 1:
                    done.append((helper, n_head + head, block, head, 1))
                done.append((helper, n_head + origin, block, origin, 1))
        for condition, slot, _, _, _ in done:
            pl.when(condition)(functools.partial(send_share, slot))
        for condition, *rest in waiting:
            pl.when(condition)(functools.partial(reduce_share, *rest))
        every += done
        waiting = done
    for condition, *rest in waiting:
        pl.when(condition)(functools.partial(reduce_share, *rest))

    home = seq // owners
    at_end = jnp.logical_and(jnp.logical_or(home == 0, home == last), head != home)
    for kind in range(2 if helps else 1):
        plane = home if kind == 0 else jnp.where(home == 0, 1, last - 1)
        for source in range(reducers):
            away = jnp.logical_not(jnp.logical_and(seq == source, head == plane))

            @pl.when(jnp.logical_and(away, at_end) if kind else away)
            def _():
                pltpu.make_async_remote_copy(
                    src_ref=final_ref.at[0, :, pl.ds(0, piece)] if piece < width else final_ref.at[0],
                    dst_ref=finals_ref.at[kind, pl.ds(source * rows_per, rows_per), :],
                    send_sem=final_send.at[0, 0], recv_sem=final_recv.at[kind, source],
                    device_id=(source, plane), device_id_type=MESH,
                ).wait_recv()
    if helps:
        @pl.when(at_end)
        def _():
            finals_ref[0] += finals_ref[1]
    per = grad_ref.shape[1]
    if per == piece:
        grad_ref[...] = finals_ref[0]
    else:
        for owner in range(owners):
            @pl.when(lax.rem(seq, owners) == owner)
            def _():
                grad_ref[...] = finals_ref[0][:, owner * per : (owner + 1) * per]

    for target in range(1, n_seq):
        @pl.when(seq < target)
        def _():
            state_copy(target).wait_send()
    for way in range(2):
        place = places[way]

        @pl.when(place == last)
        def _():
            for c in range(keep, CHUNKS):
                help_copy(way, c).wait_send()

        for distance in range(last):
            def drain(c, carry):
                @pl.when(jnp.logical_and(place >= distance, place + 1 <= limit(c)))
                def _():
                    ring_copy(way, distance, c).wait_send()
                return carry

            lax.fori_loop(0, CHUNKS, drain, 0)
    for condition, slot, block, origin, kind in every:
        @pl.when(condition)
        def _():
            for target in range(reducers):
                @pl.when(seq != target)
                def _():
                    share_copy(slot, target).wait_send()

            @pl.when(seq < reducers)
            def _():
                for owner in range(owners):
                    @pl.when(jnp.logical_not(is_self(block, origin, owner)))
                    def _():
                        final_copy(slot, block, origin, kind, owner).wait_send()
    attn_copy.wait()


def body(n_seq, n_head, queries, keys, values, level_ids, level_table, out_cotangent):
    block_len, head_dim = queries.shape
    width = out_cotangent.shape[1]
    per = width * n_head // n_seq
    piece = per if per % 128 == 0 else width
    seq_bits = n_seq.bit_length() - 1
    inner = (block_len // TILE).bit_length() - 1
    rows_per = max(16, head_dim // n_seq)
    reducers = head_dim // rows_per
    steps = max(1, n_head - 1)
    slots = 2 * n_head
    dma = pltpu.SemaphoreType.DMA
    vmem = pl.BlockSpec(memory_space=pltpu.VMEM)
    hbm = pl.BlockSpec(memory_space=pl.ANY)
    attn_out, grad = pl.pallas_call(
        functools.partial(kernel, n_seq, n_head),
        out_shape=(
            jax.ShapeDtypeStruct((block_len, head_dim), BF16),
            jax.ShapeDtypeStruct((head_dim, per), F32),
        ),
        in_specs=[hbm, hbm, hbm, vmem, vmem, hbm],
        out_specs=(hbm, vmem),
        scratch_shapes=[
            pltpu.VMEM((block_len, head_dim), BF16),
            pltpu.VMEM((block_len, head_dim), BF16),
            pltpu.VMEM((block_len, head_dim), BF16),
            pltpu.VMEM((block_len, width), BF16),
            pltpu.VMEM((TILE, TILE), jnp.int32),
            pltpu.VMEM((block_len, level_table.shape[1]), F32),
            pltpu.VMEM((block_len, head_dim), F32),
            pltpu.VMEM((block_len // TILE, head_dim, inner * head_dim), BF16),
            pltpu.VMEM((head_dim, head_dim), BF16),
            pltpu.VMEM((n_seq, head_dim, head_dim), BF16),
            pltpu.VMEM((2 * head_dim, seq_bits * head_dim), BF16),
            pltpu.VMEM((block_len, head_dim), BF16),
            pltpu.VMEM((n_head, CHUNKS, head_dim, block_len // CHUNKS), BF16),
            pltpu.VMEM((slots, head_dim, width), F32),
            pltpu.VMEM((slots, head_dim, width), BF16),
            pltpu.VMEM((slots, n_seq, rows_per, width), BF16),
            pltpu.VMEM((slots, rows_per, width), F32),
            pltpu.VMEM((2, head_dim, piece), F32),
            pltpu.VMEM((CHUNKS - KEEP, block_len // CHUNKS, width), BF16),
            dma((4,)),
            dma((1,)),
            dma((n_seq,)),
            dma((n_seq,)),
            dma((2, steps, CHUNKS)),
            dma((2, steps, CHUNKS)),
            dma((slots, reducers)),
            dma((slots, n_seq)),
            dma((slots, n_seq // n_head)),
            dma((2, reducers)),
            dma((CHUNKS - KEEP,)),
            dma((CHUNKS - KEEP,)),
        ],
        compiler_params=pltpu.CompilerParams(
            collective_id=0, has_side_effects=True, vmem_limit_bytes=60 * 2**20
        ),
    )(queries, keys, values, level_ids[None, :], level_table.T, out_cotangent)
    return attn_out, grad.T


def solution(mesh):
    in_specs = (
        P("seq", "head"),
        P("seq", "head"),
        P("seq", "head"),
        P("seq"),
        P(),
        P("seq", "head"),
    )
    out_specs = (P("seq", "head"), P("seq", "head"))
    return jax.shard_map(
        functools.partial(body, mesh.shape["seq"], mesh.shape["head"]),
        mesh=mesh, in_specs=in_specs, out_specs=out_specs, check_vma=False,
    )
```
